32 devices in a mesh: gx: 8 (over y, x, core), gy: 4 (over z).
Axes of the slice: x: 2, y: 2, z: 4, core: 2. Of those that a mesh axis runs over, the one named last changes fastest.
Arguments:
- date_key: int32 [393216], P(('gx', 'gy')), may hold values from 0 to 4095
- store_key: int32 [393216], P(('gx', 'gy')), may hold values from 0 to 65535
- product_key: int32 [393216], P(('gx', 'gy')), may hold values from 0 to 1048575
- revenue: bfloat16 [393216], P(('gx', 'gy')), may hold values from -0.59765625 to 0.59765625
- row_counts: int32 [32], P(('gx', 'gy')), may hold values from 1 to 12288, 245760 in all
- date_years: int32 [512], P('gx'), may hold values from -2147483648 to 2147483646
- date_flags: int32 [128], P('gx'), may hold values from -2147483648 to 2147483646
- store_flags: int32 [2048], P('gx'), may hold values from -2147483648 to 2147483646
- product_flags: int32 [32768], P('gx'), may hold values from -2147483648 to 2147483646
- brand_words: int32 [349568], P('gx'), may hold values from 0 to 1073741823
Outputs:
- revenue_groups: float32 [16, 1024], replicated
The draws below stay inside these ranges and needn't reach their ends.
Inputs may be any that keep to these rules, and one draw needn't show every extreme that they name: Rows d * 12288 to d * 12288 + row_counts[d] - 1 of the fact arrays are live; the largest count equals 12288. `date_years`: date k's year code is in bits 4 * (k % 8) of word k // 8. `date_flags`: bit k % 32 of word k // 32 is the flag of row k. `store_flags`: bit k % 32 of word k // 32 is the flag of row k. `product_flags`: bit k % 32 of word k // 32 is the flag of row k. `brand_words`: product with shard o and local index l holds its brand code in bits 10 * (l % 3) of word o * 43696 + l // 3; words past a shard's products are unused.
All inputs are finite; a program needn't handle non-finite values. No bound on the sum of `row_counts` on one device may be relied on, other than what follows from the above.
Results may differ from the reference program's by a relative error of at most 0.0003.
Values sent between devices are 32-bit elements; how exact they have to be, the bound alone decides.
A program may use at most 64 MiB of HBM per device.

```python
import math
import jax
import jax.numpy as jnp
import numpy as np

DATES = 4096
STORES = 65536
PRODUCTS = 1048576
BRANDS = 1024
YEARS = 16
FACT_DEV = 12288
BW_DEV = 43696
N_GX = 8
N_GY = 4
DEVICES = 32


def touch_ends(drawn, rng, low, high):
    spot = [jax.random.randint(jax.random.fold_in(rng, axis), (), 0, length) for axis, length in enumerate(drawn.shape)]
    main_axis = drawn.shape.index(max(drawn.shape))
    neighbour = spot[:main_axis] + [(spot[main_axis] + 1) % drawn.shape[main_axis]] + spot[main_axis + 1:]
    return drawn.at[tuple(spot)].set(low).at[tuple(neighbour)].set(high)


def levels(stream_key, dims, shards, least, high):
    def one(axis_at, shards_of):
        draws = jax.random.uniform(jax.random.fold_in(jax.random.fold_in(stream_key, 6), axis_at), (shards_of,), jnp.float32, least / len(shards), high / len(shards))
        return jnp.repeat(jnp.exp(draws), dims[axis_at] // shards_of).reshape((-1,) + (1,) * (len(dims) - axis_at - 1))

    gain = one(*shards[0])
    for cut in shards[1:]:
        gain = gain * one(*cut)
    return gain


def wide_ids(stream_key, dims, count, skew):
    loads = [min(1 << octave, count + 1 - (1 << octave)) * (1 << 20) // math.isqrt((1 << octave) ** skew) + 1 for octave in range((count + 1).bit_length()) if 1 << octave <= count]
    width = 1 + sum(loads) // (1 << 30)
    table = np.cumsum(np.array([max(1, weight // width) for weight in loads]))
    ticket = jax.random.randint(jax.random.fold_in(stream_key, 1), dims, 0, int(table[len(loads) - 1]))
    start = jnp.left_shift(1, jnp.searchsorted(jnp.asarray(table, jnp.int32), ticket, side="right").astype(jnp.int32))
    standing = start - 1 + jax.random.randint(jax.random.fold_in(stream_key, 4), dims, 0, 1 << 30) % jnp.minimum(start, count + 1 - start)
    return jax.random.permutation(jax.random.fold_in(stream_key, 2), count)[standing].astype(jnp.int32)


def length_profile(number_of, total, most, lean):
    weights = [(1 << 20) // math.isqrt(standing ** lean) + 1 for standing in range(2, number_of + 1)]
    spare, counts = total - most - (number_of - 1), [1] * (number_of - 1)
    while spare > 0:
        free = [i for i in range(number_of - 1) if counts[i] < most]
        pool, remaining = sum([weights[i] for i in free]), spare
        for i in free:
            extra = min(most - counts[i], max(1, remaining * weights[i] // pool), spare)
            counts[i] = counts[i] + extra
            spare = spare - extra
    return np.array([most] + counts)


def uneven_parts(own_key, count, total, most, slope):
    if count == 2:
        one = jax.random.randint(own_key, (), max(1, total - most), min(most, total - 1) + 1)
        return jnp.stack([one, total - one])
    lengths = jnp.asarray(length_profile(count, total, most, slope), jnp.int32)
    couples = (count - 1) // 2
    giver, sink = lengths[1:1 + 2 * couples:2], lengths[2:2 + 2 * couples:2]
    slack = jnp.minimum(giver - 1, most - sink)
    moved = jax.random.randint(jax.random.fold_in(own_key, 1), (couples,), 0, 1 << 20) % (slack + 1)
    lengths = lengths.at[1:1 + 2 * couples:2].set(giver - moved).at[2:2 + 2 * couples:2].set(sink + moved)
    return lengths[jax.random.permutation(jax.random.fold_in(own_key, 2), count)]


def normal_values(rng, extent, spread, most, pieces=(), kind=jnp.bfloat16):
    loudness = levels(rng, extent, pieces, -0.22, 0.18) if pieces else 1.0
    drawn = jax.random.normal(rng, extent, jnp.float32) * spread * loudness
    return jnp.minimum(jnp.maximum(drawn, -most), most).astype(kind)


def setup_inputs(seed: int = 0) -> dict:
    streams_of = jax.random.split(jax.random.key(seed), 11)
    date_key = touch_ends(jax.random.randint(streams_of[0], (FACT_DEV * DEVICES,), 0, DATES), jax.random.fold_in(streams_of[0], 1), 0, DATES - 1).astype(jnp.int32)
    store_key = touch_ends(jax.random.randint(streams_of[1], (FACT_DEV * DEVICES,), 0, STORES), jax.random.fold_in(streams_of[1], 1), 0, STORES - 1).astype(jnp.int32)
    product_key = touch_ends(wide_ids(streams_of[2], (FACT_DEV * DEVICES,), PRODUCTS, 1), jax.random.fold_in(streams_of[2], 3), 0, PRODUCTS - 1).astype(jnp.int32)
    revenue = normal_values(streams_of[3], (FACT_DEV * DEVICES,), 0.1, 0.59765625, ((0, 32),))
    row_counts = uneven_parts(streams_of[4], DEVICES, DEVICES * FACT_DEV * 5 // 8, FACT_DEV, 2).astype(jnp.int32)
    date_years = touch_ends(jax.random.randint(streams_of[5], (DATES // 8,), -2147483648, 2147483647), jax.random.fold_in(streams_of[5], 1), -2147483648, 2147483646).astype(jnp.int32)
    date_flags = touch_ends(jax.random.randint(streams_of[6], (DATES // 32,), -2147483648, 2147483647), jax.random.fold_in(streams_of[6], 1), -2147483648, 2147483646).astype(jnp.int32)
    store_flags = touch_ends(jax.random.randint(streams_of[7], (STORES // 32,), -2147483648, 2147483647), jax.random.fold_in(streams_of[7], 1), -2147483648, 2147483646).astype(jnp.int32)
    product_flags = touch_ends(jax.random.randint(streams_of[8], (PRODUCTS // 32,), -2147483648, 2147483647), jax.random.fold_in(streams_of[8], 1), -2147483648, 2147483646).astype(jnp.int32)
    brand_words = touch_ends(jax.random.randint(streams_of[9], (BW_DEV * N_GX,), 0, 1073741824), jax.random.fold_in(streams_of[9], 1), 0, 1073741823).astype(jnp.int32)
    return dict(date_key=date_key, store_key=store_key, product_key=product_key, revenue=revenue, row_counts=row_counts, date_years=date_years, date_flags=date_flags, store_flags=store_flags, product_flags=product_flags, brand_words=brand_words)


def pick_bits(packed, position, width_bits):
    per_word = 32 // width_bits
    chosen = packed[position // per_word]
    shifted = jnp.right_shift(chosen, (position % per_word) * width_bits)
    return jnp.bitwise_and(shifted, (1 << width_bits) - 1)


def reference(date_key, store_key, product_key, revenue, row_counts, date_years, date_flags, store_flags, product_flags, brand_words):
    prod_shard = PRODUCTS // N_GX
    positions = jnp.arange(FACT_DEV * N_GX * N_GY, dtype=jnp.int32)
    live_rows = (positions % FACT_DEV) < row_counts[positions // FACT_DEV]
    year_code = pick_bits(date_years, date_key, 4)
    passed = pick_bits(date_flags, date_key, 1) * pick_bits(store_flags, store_key, 1) * pick_bits(product_flags, product_key, 1)
    owner_idx = product_key // prod_shard
    local_idx = product_key % prod_shard
    word_val = brand_words[owner_idx * BW_DEV + local_idx // 3]
    brand_code = jnp.bitwise_and(jnp.right_shift(word_val, (local_idx % 3) * 10), 1023)
    kept_rows = live_rows & (passed == 1)
    amount = jnp.where(kept_rows, revenue.astype(jnp.float32), jnp.float32(0))
    group_id = year_code * BRANDS + brand_code
    totals = jax.ops.segment_sum(amount, group_id, num_segments=YEARS * BRANDS)
    return totals.reshape(YEARS, BRANDS)
```

```python
import functools

import jax
import jax.numpy as jnp
from jax import lax
from jax.experimental import pallas as pl
from jax.experimental.pallas import tpu as pltpu
from jax.sharding import PartitionSpec as P

BRANDS = 1024
YEARS = 16
LANES = 128
GROUP = 4
MESH = pl.DeviceIdType.MESH
VMEM = pl.BlockSpec(memory_space=pltpu.VMEM)
SMEM = pl.BlockSpec(memory_space=pltpu.SMEM)


def up(count, unit):
    return (count + unit - 1) // unit * unit


def flip(me, mask):
    out, bit = me, 1
    while bit <= mask:
        if mask & bit:
            out = out + bit * (1 - 2 * ((me // bit) % 2))
        bit *= 2
    return out


def spread_kernel(n, x_ref, o_ref, own_sem, send_sem, recv_sem):
    me = lax.axis_index("gx")
    half = x_ref.shape[0] // 2
    bits = n.bit_length() - 1
    rising = [1 << b for b in range(1, bits)]
    orders = (rising + [1], rising[::-1] + [1])
    barrier = pltpu.get_barrier_semaphore()
    for b in range(bits):
        pl.semaphore_signal(barrier, inc=1, device_id={"gx": flip(me, 1 << b)}, device_id_type=MESH)
    own = pltpu.make_async_copy(x_ref, o_ref.at[me], own_sem)
    own.start()
    pl.semaphore_wait(barrier, bits)

    def copy(h, mask, step):
        rows = pl.ds(h * half, half)
        slot = flip(me, mask)
        src = x_ref.at[rows] if mask == 0 else o_ref.at[slot, rows]
        return pltpu.make_async_remote_copy(
            src_ref=src,
            dst_ref=o_ref.at[slot, rows],
            send_sem=send_sem.at[h, mask + step],
            recv_sem=recv_sem.at[h, mask + step],
            device_id={"gx": flip(me, step)},
            device_id_type=MESH,
        )

    sent = []
    for h in range(2):
        for step in orders[h]:
            c = copy(h, 0, step)
            c.start()
            sent.append(c)
    arrivals = []
    for h in range(2):
        have = [0]
        listed = []
        for step in orders[h]:
            fresh = [m + step for m in have]
            listed += [(m, step) for m in fresh]
            have += fresh
        arrivals.append(listed)
    for pair in zip(*arrivals):
        for h, (mask, last) in enumerate(pair):
            copy(h, mask - last, last).wait_recv()
            for step in orders[h][orders[h].index(last) + 1:]:
                c = copy(h, mask, step)
                c.start()
                sent.append(c)
    for c in sent:
        c.wait_send()
    own.wait()


def spread(n, table):
    return pl.pallas_call(
        functools.partial(spread_kernel, n),
        out_shape=jax.ShapeDtypeStruct((n,) + table.shape, jnp.int32),
        in_specs=[VMEM],
        out_specs=VMEM,
        scratch_shapes=[
            pltpu.SemaphoreType.DMA,
            pltpu.SemaphoreType.DMA((2, n)),
            pltpu.SemaphoreType.DMA((2, n)),
        ],
        compiler_params=pltpu.CompilerParams(collective_id=0, has_side_effects=True),
    )(table)


def scan(tab_ref, n, base, rows, keys):
    unit = min(8, rows)

    def tile(code, first, owner, acc):
        out = list(acc)
        for r in range(unit):
            words = jnp.broadcast_to(tab_ref[owner, pl.ds(first + r, 1), :], (8, LANES))
            for v, (high, lane) in enumerate(keys):
                got = jnp.take_along_axis(words, lane, axis=1, mode="promise_in_bounds")
                out[v] = jnp.where(high == code + r, got, out[v])
        return tuple(out)

    def per_owner(owner, acc):
        if rows == unit:
            return tile(owner * rows, base, owner, acc)
        return lax.fori_loop(
            0, rows // unit, lambda t, a: tile(owner * rows + t * unit, base + t * unit, owner, a), acc
        )

    zero = tuple(jnp.zeros((8, LANES), jnp.int32) for _ in keys)
    return list(lax.fori_loop(0, n, per_owner, zero))


def local_kernel(n, places, count_ref, date_ref, store_ref, product_ref, money_ref, tab_ref, o_ref,
                 word_buf, money_buf):
    tall = date_ref.shape[0]
    tiles = tall // 8
    (year_base, year_rows, year_words), (dflag_base, dflag_rows, dflag_words) = places[:2]
    (store_base, store_rows, store_words), (prod_base, prod_rows, prod_words) = places[2:4]
    brand_base, brand_rows, _ = places[4]

    def split(ref):
        return [ref[pl.ds(8 * v, 8), :] for v in range(tiles)]

    def keyed(word, per_shard, rows):
        owner, inside = word // per_shard, word % per_shard
        return owner * rows + inside // LANES, inside % LANES

    def where_is(keys, shift, words, rows):
        out = []
        for k in keys:
            w = lax.shift_right_logical(k, shift)
            owner = lax.shift_right_logical(w, words.bit_length() - 1)
            inside = w & (words - 1)
            out.append((owner * rows + lax.shift_right_logical(inside, 7), inside & (LANES - 1)))
        return out

    dates, stores, products = split(date_ref), split(store_ref), split(product_ref)
    year_word = scan(tab_ref, n, year_base, year_rows, where_is(dates, 3, year_words, year_rows))
    date_word = scan(tab_ref, n, dflag_base, dflag_rows, where_is(dates, 5, dflag_words, dflag_rows))
    store_word = scan(tab_ref, n, store_base, store_rows, where_is(stores, 5, store_words, store_rows))
    prod_word = scan(tab_ref, n, prod_base, prod_rows, where_is(products, 5, prod_words, prod_rows))
    count = count_ref[0]
    spot = lax.broadcasted_iota(jnp.int32, (8, LANES), 0) * LANES + lax.broadcasted_iota(
        jnp.int32, (8, LANES), 1
    )
    keep, packed = [], []
    for v in range(tiles):
        year = lax.shift_right_logical(year_word[v], (dates[v] & 7) * 4) & 15
        passed = lax.shift_right_logical(date_word[v], dates[v] & 31)
        passed &= lax.shift_right_logical(store_word[v], stores[v] & 31)
        passed &= lax.shift_right_logical(prod_word[v], products[v] & 31)
        passed &= 1
        keep.append(jnp.where(spot + v * 8 * LANES < count, passed, 0))
        packed.append(products[v] | (year << 20))
    keep = jnp.concatenate(keep, axis=0)
    packed = jnp.concatenate(packed, axis=0)
    row = lax.broadcasted_iota(jnp.int32, (tall, LANES), 0)

    upto = keep
    step = 1
    while step < tall:
        upto = upto + jnp.where(row >= step, pltpu.roll(upto, step, 0), 0)
        step *= 2
    most = jnp.max(upto[tall - 8:, :])
    word = jnp.where(keep == 1, packed | ((row - upto + 1) << 24), -1)
    money = jnp.where(keep == 1, money_ref[...], 0.0)
    step, bit = 1, 24
    while step < tall:
        far_word = pltpu.roll(word, tall - step, 0)
        far_money = pltpu.roll(money, tall - step, 0)
        comes = (far_word >= 0) & ((far_word & (1 << bit)) != 0)
        leaves = (word & (1 << bit)) != 0
        word = jnp.where(comes, far_word, jnp.where(leaves, -1, word))
        money = jnp.where(comes, far_money, jnp.where(leaves, 0.0, money))
        step *= 2
        bit += 1
    word_buf[...] = word
    money_buf[...] = money
    o_ref[...] = jnp.zeros_like(o_ref)

    shard_bits = (prod_words * 32).bit_length() - 1
    group_row = lax.broadcasted_iota(jnp.int32, (LANES, LANES), 0)

    def group(g, carry):
        keys, shifts, years = [], [], []
        for v in range(GROUP):
            w = word_buf[pl.ds(pl.multiple_of(g * GROUP * 8 + v * 8, 8), 8), :]
            key = w & 0xFFFFF
            owner = lax.shift_right_logical(key, shard_bits)
            inside = key & ((1 << shard_bits) - 1)
            third = ((inside.astype(jnp.float32) + 0.5) * (1.0 / 3.0)).astype(jnp.int32)
            shifts.append((inside - third * 3) * 10)
            keys.append((owner * brand_rows + lax.shift_right_logical(third, 7), third & (LANES - 1)))
            years.append(lax.shift_right_logical(w, 20) & 15)
        words = scan(tab_ref, n, brand_base, brand_rows, keys)
        total = o_ref[...]
        for v in range(GROUP):
            brand = lax.shift_right_logical(words[v], shifts[v]) & 1023
            high = lax.shift_right_logical(brand, 7) * YEARS + years[v]
            low = brand & (LANES - 1)
            cash = money_buf[pl.ds(pl.multiple_of(g * GROUP * 8 + v * 8, 8), 8), :]
            left, right = [], []
            for s in range(8):
                left.append(jnp.where(group_row == high[s:s + 1], cash[s:s + 1], 0.0).astype(jnp.bfloat16))
                right.append(jnp.where(group_row == low[s:s + 1], 1.0, 0.0).astype(jnp.bfloat16))
            total = total + lax.dot_general(
                jnp.concatenate(left, axis=1), jnp.concatenate(right, axis=1),
                (((1,), (1,)), ((), ())), preferred_element_type=jnp.float32,
            )
        o_ref[...] = total
        return carry

    lax.fori_loop(0, (most + GROUP * 8 - 1) // (GROUP * 8), group, 0)


def local(n, places, count, date, store, product, money, tables):
    tall = date.shape[0]
    return pl.pallas_call(
        functools.partial(local_kernel, n, places),
        out_shape=jax.ShapeDtypeStruct((LANES, LANES), jnp.float32),
        in_specs=[SMEM] + [VMEM] * 5,
        out_specs=VMEM,
        scratch_shapes=[pltpu.VMEM((tall, LANES), jnp.int32), pltpu.VMEM((tall, LANES), jnp.float32)],
    )(count, date, store, product, money, tables)


def join_kernel(nx, ny, x_ref, o_ref, in_x, part, in_y, whole, sx, rx, sy, ry, sz, rz):
    mx, my = lax.axis_index("gx"), lax.axis_index("gy")
    rows = part.shape[0]
    barrier = pltpu.get_barrier_semaphore()
    for d in range(1, nx):
        pl.semaphore_signal(barrier, inc=1, device_id={"gx": (mx + d) % nx}, device_id_type=MESH)
    for d in range(1, ny):
        pl.semaphore_signal(barrier, inc=1, device_id={"gy": (my + d) % ny}, device_id_type=MESH)
    pl.semaphore_wait(barrier, nx + ny - 2)

    def push(src, dst, send, recv, where):
        c = pltpu.make_async_remote_copy(
            src_ref=src, dst_ref=dst, send_sem=send, recv_sem=recv, device_id=where, device_id_type=MESH
        )
        c.start()
        return c

    first = []
    for d in range(1, nx):
        to = (mx + d) % nx
        first.append(push(x_ref.at[to], in_x.at[d - 1], sx.at[d - 1], rx.at[d - 1], {"gx": to}))
    total = x_ref[mx]
    for d, c in enumerate(first):
        c.wait_recv()
        total = total + in_x[d]
    part[...] = total
    second = []
    for d in range(1, ny):
        second.append(push(part, in_y.at[(my)], sy.at[d - 1], ry.at[d - 1], {"gy": (my + d) % ny}))
    for c in second:
        c.wait_recv()
    in_y[my] = total
    total = in_y[0]
    for d in range(1, ny):
        total = total + in_y[d]
    whole[mx] = total
    third = []
    for d in range(1, nx):
        third.append(push(whole.at[mx], whole.at[mx], sz.at[d - 1], rz.at[d - 1], {"gx": (mx + d) % nx}))
    for c in third:
        c.wait_recv()
    flat = whole[...].reshape(nx * rows, LANES)
    for j in range(BRANDS // LANES):
        o_ref[:, j * LANES:(j + 1) * LANES] = flat[j * YEARS:(j + 1) * YEARS]
    for c in first + second + third:
        c.wait_send()


def join(nx, ny, sums):
    rows = LANES // nx
    dma = pltpu.SemaphoreType.DMA
    return pl.pallas_call(
        functools.partial(join_kernel, nx, ny),
        out_shape=jax.ShapeDtypeStruct((YEARS, BRANDS), jnp.float32),
        in_specs=[VMEM],
        out_specs=VMEM,
        scratch_shapes=[
            pltpu.VMEM((nx - 1, rows, LANES), jnp.float32),
            pltpu.VMEM((rows, LANES), jnp.float32),
            pltpu.VMEM((ny, rows, LANES), jnp.float32),
            pltpu.VMEM((nx, rows, LANES), jnp.float32),
            dma((nx,)), dma((nx,)), dma((ny,)), dma((ny,)), dma((nx,)), dma((nx,)),
        ],
        compiler_params=pltpu.CompilerParams(collective_id=1, has_side_effects=True),
    )(sums.reshape(nx, rows, LANES))


def shards(nx, ny, date_key, store_key, product_key, revenue, row_counts,
           date_years, date_flags, store_flags, product_flags, brand_words):
    sections = [None] * 5
    pieces, base = [], 0
    tables = (date_years, date_flags, store_flags, product_flags, brand_words)
    for at in (4, 3, 2, 1, 0):
        words = tables[at].shape[0]
        rows = up(words, LANES) // LANES
        rows = up(rows, 8) if rows > 8 else rows
        sections[at] = (base, rows, words)
        pieces.append(jnp.pad(tables[at], (0, rows * LANES - words)))
        base += rows
    tail = up(base, 16) - base
    if tail:
        pieces.append(jnp.zeros((tail * LANES,), jnp.int32))
    table = jnp.concatenate(pieces).reshape(base + tail, LANES)
    tabs = spread(nx, table)
    flat = lambda a: a.reshape(-1, LANES)
    sums = local(nx, tuple(sections), row_counts, flat(date_key), flat(store_key), flat(product_key),
                 flat(revenue.astype(jnp.float32)), tabs)
    return join(nx, ny, sums)


def solution(mesh):
    rows = P(("gx", "gy"))
    return jax.shard_map(
        functools.partial(shards, mesh.shape["gx"], mesh.shape["gy"]),
        mesh=mesh,
        in_specs=(rows,) * 5 + (P("gx"),) * 5,
        out_specs=P(),
        check_vma=False,
    )
```

```python
import functools

import jax
import jax.numpy as jnp
from jax import lax
from jax.experimental import pallas as pl
from jax.experimental.pallas import tpu as pltpu
from jax.sharding import PartitionSpec as P

BRANDS = 1024
YEARS = 16
LANES = 128
MESH = pl.DeviceIdType.MESH
VMEM = pl.BlockSpec(memory_space=pltpu.VMEM)
SMEM = pl.BlockSpec(memory_space=pltpu.SMEM)


def up(count, unit):
    return (count + unit - 1) // unit * unit


def flip(me, mask):
    out, bit = me, 1
    while bit <= mask:
        if mask & bit:
            out = out + bit * (1 - 2 * ((me // bit) % 2))
        bit *= 2
    return out


def spread_kernel(n, x_ref, o_ref, own_sem, send_sem, recv_sem):
    me = lax.axis_index("gx")
    half = x_ref.shape[0] // 2
    bits = n.bit_length() - 1
    rising = [1 << b for b in range(1, bits)]
    orders = (rising + [1], rising[::-1] + [1])
    barrier = pltpu.get_barrier_semaphore()
    for b in range(bits):
        pl.semaphore_signal(barrier, inc=1, device_id={"gx": flip(me, 1 << b)}, device_id_type=MESH)
    own = pltpu.make_async_copy(x_ref, o_ref.at[me], own_sem)
    own.start()
    pl.semaphore_wait(barrier, bits)

    def copy(h, mask, step):
        rows = pl.ds(h * half, half)
        slot = flip(me, mask)
        src = x_ref.at[rows] if mask == 0 else o_ref.at[slot, rows]
        return pltpu.make_async_remote_copy(
            src_ref=src,
            dst_ref=o_ref.at[slot, rows],
            send_sem=send_sem.at[h, mask + step],
            recv_sem=recv_sem.at[h, mask + step],
            device_id={"gx": flip(me, step)},
            device_id_type=MESH,
        )

    sent = []
    for h in range(2):
        for step in orders[h]:
            c = copy(h, 0, step)
            c.start()
            sent.append(c)
    arrivals = []
    for h in range(2):
        have = [0]
        listed = []
        for step in orders[h]:
            fresh = [m + step for m in have]
            listed += [(m, step) for m in fresh]
            have += fresh
        arrivals.append(listed)
    for pair in zip(*arrivals):
        for h, (mask, last) in enumerate(pair):
            copy(h, mask - last, last).wait_recv()
            for step in orders[h][orders[h].index(last) + 1:]:
                c = copy(h, mask, step)
                c.start()
                sent.append(c)
    for c in sent:
        c.wait_send()
    own.wait()


def spread(n, table):
    return pl.pallas_call(
        functools.partial(spread_kernel, n),
        out_shape=jax.ShapeDtypeStruct((n,) + table.shape, jnp.int32),
        in_specs=[VMEM],
        out_specs=VMEM,
        scratch_shapes=[
            pltpu.SemaphoreType.DMA,
            pltpu.SemaphoreType.DMA((2, n)),
            pltpu.SemaphoreType.DMA((2, n)),
        ],
        compiler_params=pltpu.CompilerParams(collective_id=0, has_side_effects=True),
    )(table)


DIMS = lax.GatherDimensionNumbers(
    offset_dims=(), collapsed_slice_dims=(1,), start_index_map=(1,),
    operand_batching_dims=(0,), start_indices_batching_dims=(0,),
)


def along_lanes(words, lane):
    return lax.gather(words, lane[..., None], DIMS, (1, 1), mode=lax.GatherScatterMode.PROMISE_IN_BOUNDS)


def pick(tab_ref, owner, base, rows, high, lane):
    parts = [jnp.zeros((8, LANES), jnp.int32) for _ in range(4)]
    mine = high - owner * rows
    for r in range(rows):
        words = jnp.broadcast_to(tab_ref[owner, pl.ds(base + r, 1), :], (8, LANES))
        parts[r % 4] = jnp.where(mine == r, along_lanes(words, lane), parts[r % 4])
    return (parts[0] | parts[1]) | (parts[2] | parts[3])


def local_kernel(n, places, count_ref, date_ref, store_ref, product_ref, money_ref, tab_ref, o_ref,
                 word_buf, money_buf):
    tall = date_ref.shape[0]
    tiles = tall // 8
    (year_base, year_rows, year_words), (dflag_base, dflag_rows, dflag_words) = places[:2]
    (store_base, store_rows, store_words), (prod_base, prod_rows, prod_words) = places[2:4]
    brand_base, brand_rows, _ = places[4]

    def where_is(k, shift, words, rows):
        w = lax.shift_right_logical(k, shift)
        owner = lax.shift_right_logical(w, words.bit_length() - 1)
        inside = w & (words - 1)
        return owner * rows + lax.shift_right_logical(inside, 7), inside & (LANES - 1)

    def look(keys, shift, base, rows, words):
        high, lane = where_is(keys, shift, words, rows)
        if n * rows <= 512:
            out = jnp.zeros((8, LANES), jnp.int32)
            for owner in range(n):
                out = out | pick(tab_ref, owner, base, rows, high, lane)
            return out
        return lax.fori_loop(
            0, n, lambda o, acc: acc | pick(tab_ref, o, base, rows, high, lane), jnp.zeros((8, LANES), jnp.int32)
        )

    count = count_ref[0]
    spot = lax.broadcasted_iota(jnp.int32, (8, LANES), 0) * LANES + lax.broadcasted_iota(
        jnp.int32, (8, LANES), 1
    )

    def filter_tile(v, carry):
        at = pl.ds(pl.multiple_of(v * 8, 8), 8)
        date, store, product = date_ref[at, :], store_ref[at, :], product_ref[at, :]
        year = lax.shift_right_logical(look(date, 3, year_base, year_rows, year_words), (date & 7) * 4) & 15
        passed = lax.shift_right_logical(look(date, 5, dflag_base, dflag_rows, dflag_words), date & 31)
        passed &= lax.shift_right_logical(look(store, 5, store_base, store_rows, store_words), store & 31)
        passed &= lax.shift_right_logical(look(product, 5, prod_base, prod_rows, prod_words), product & 31)
        live = spot + v * (8 * LANES) < count
        word_buf[at, :] = jnp.where(live & ((passed & 1) == 1), product | (year << 20), -1)
        return carry

    lax.fori_loop(0, tiles, filter_tile, 0)
    packed = word_buf[...]
    keep = (packed >= 0).astype(jnp.int32)
    row = lax.broadcasted_iota(jnp.int32, (tall, LANES), 0)

    upto = keep
    step = 1
    while step < tall:
        upto = upto + jnp.where(row >= step, pltpu.roll(upto, step, 0), 0)
        step *= 2
    most = jnp.max(upto[tall - 8:, :])
    word = jnp.where(keep == 1, packed | ((row - upto + 1) << 24), -1)
    money = jnp.where(keep == 1, money_ref[...], 0.0)
    step, bit = 1, 24
    while step < tall:
        far_word = pltpu.roll(word, tall - step, 0)
        far_money = pltpu.roll(money, tall - step, 0)
        comes = (far_word >= 0) & ((far_word & (1 << bit)) != 0)
        leaves = (word & (1 << bit)) != 0
        word = jnp.where(comes, far_word, jnp.where(leaves, -1, word))
        money = jnp.where(comes, far_money, jnp.where(leaves, 0.0, money))
        step *= 2
        bit += 1
    word_buf[...] = word
    money_buf[...] = money
    o_ref[...] = jnp.zeros_like(o_ref)

    shard_bits = (prod_words * 32).bit_length() - 1
    group_row = lax.broadcasted_iota(jnp.int32, (LANES, LANES), 0)

    def group(g, carry):
        at = pl.ds(pl.multiple_of(g * 8, 8), 8)
        w = word_buf[at, :]
        cash = money_buf[at, :]
        key = w & 0xFFFFF
        owner = lax.shift_right_logical(key, shard_bits)
        inside = key & ((1 << shard_bits) - 1)
        third = ((inside.astype(jnp.float32) + 0.5) * (1.0 / 3.0)).astype(jnp.int32)
        shift = (inside - third * 3) * 10
        high = owner * brand_rows + lax.shift_right_logical(third, 7)
        lane = third & (LANES - 1)
        words = lax.fori_loop(
            0, n, lambda o, acc: acc | pick(tab_ref, o, brand_base, brand_rows, high, lane),
            jnp.zeros((8, LANES), jnp.int32),
        )
        brand = lax.shift_right_logical(words, shift) & 1023
        row_code = lax.shift_right_logical(brand, 7) * YEARS + (lax.shift_right_logical(w, 20) & 15)
        low = brand & (LANES - 1)
        left, right = [], []
        for s in range(8):
            left.append(jnp.where(group_row == row_code[s:s + 1], cash[s:s + 1], 0.0).astype(jnp.bfloat16))
            right.append(jnp.where(group_row == low[s:s + 1], 1.0, 0.0).astype(jnp.bfloat16))
        o_ref[...] += lax.dot_general(
            jnp.concatenate(left, axis=1), jnp.concatenate(right, axis=1),
            (((1,), (1,)), ((), ())), preferred_element_type=jnp.float32,
        )
        return carry

    lax.fori_loop(0, (most + 7) // 8, group, 0)


def local(n, places, count, date, store, product, money, tables):
    tall = date.shape[0]
    return pl.pallas_call(
        functools.partial(local_kernel, n, places),
        out_shape=jax.ShapeDtypeStruct((LANES, LANES), jnp.float32),
        in_specs=[SMEM] + [VMEM] * 5,
        out_specs=VMEM,
        scratch_shapes=[pltpu.VMEM((tall, LANES), jnp.int32), pltpu.VMEM((tall, LANES), jnp.float32)],
    )(count, date, store, product, money, tables)


def join_kernel(nx, ny, x_ref, o_ref, in_x, part, in_y, whole, sx, rx, sy, ry, sz, rz):
    mx, my = lax.axis_index("gx"), lax.axis_index("gy")
    rows = part.shape[0]
    barrier = pltpu.get_barrier_semaphore()
    for d in range(1, nx):
        pl.semaphore_signal(barrier, inc=1, device_id={"gx": (mx + d) % nx}, device_id_type=MESH)
    for d in range(1, ny):
        pl.semaphore_signal(barrier, inc=1, device_id={"gy": (my + d) % ny}, device_id_type=MESH)
    pl.semaphore_wait(barrier, nx + ny - 2)

    def push(src, dst, send, recv, where):
        c = pltpu.make_async_remote_copy(
            src_ref=src, dst_ref=dst, send_sem=send, recv_sem=recv, device_id=where, device_id_type=MESH
        )
        c.start()
        return c

    first = []
    for d in range(1, nx):
        to = (mx + d) % nx
        first.append(push(x_ref.at[to], in_x.at[d - 1], sx.at[d - 1], rx.at[d - 1], {"gx": to}))
    total = x_ref[mx]
    for d, c in enumerate(first):
        c.wait_recv()
        total = total + in_x[d]
    part[...] = total
    second = []
    for d in range(1, ny):
        second.append(push(part, in_y.at[(my)], sy.at[d - 1], ry.at[d - 1], {"gy": (my + d) % ny}))
    for c in second:
        c.wait_recv()
    in_y[my] = total
    total = in_y[0]
    for d in range(1, ny):
        total = total + in_y[d]
    whole[mx] = total
    third = []
    for d in range(1, nx):
        third.append(push(whole.at[mx], whole.at[mx], sz.at[d - 1], rz.at[d - 1], {"gx": (mx + d) % nx}))
    for c in third:
        c.wait_recv()
    flat = whole[...].reshape(nx * rows, LANES)
    for j in range(BRANDS // LANES):
        o_ref[:, j * LANES:(j + 1) * LANES] = flat[j * YEARS:(j + 1) * YEARS]
    for c in first + second + third:
        c.wait_send()


def join(nx, ny, sums):
    rows = LANES // nx
    dma = pltpu.SemaphoreType.DMA
    return pl.pallas_call(
        functools.partial(join_kernel, nx, ny),
        out_shape=jax.ShapeDtypeStruct((YEARS, BRANDS), jnp.float32),
        in_specs=[VMEM],
        out_specs=VMEM,
        scratch_shapes=[
            pltpu.VMEM((nx - 1, rows, LANES), jnp.float32),
            pltpu.VMEM((rows, LANES), jnp.float32),
            pltpu.VMEM((ny, rows, LANES), jnp.float32),
            pltpu.VMEM((nx, rows, LANES), jnp.float32),
            dma((nx,)), dma((nx,)), dma((ny,)), dma((ny,)), dma((nx,)), dma((nx,)),
        ],
        compiler_params=pltpu.CompilerParams(collective_id=1, has_side_effects=True),
    )(sums.reshape(nx, rows, LANES))


def shards(nx, ny, date_key, store_key, product_key, revenue, row_counts,
           date_years, date_flags, store_flags, product_flags, brand_words):
    sections = [None] * 5
    base = 0
    tables = (date_years, date_flags, store_flags, product_flags, brand_words)
    for at in (4, 3, 2, 1, 0):
        words = tables[at].shape[0]
        rows = up(words, LANES) // LANES
        rows = up(rows, 8) if rows > 8 else rows
        sections[at] = (base, rows, words)
        base += rows
    tall = up(base, 16)
    table = jnp.zeros((tall * LANES,), jnp.int32)
    for at in range(5):
        first, _, words = sections[at]
        table = table | jnp.pad(tables[at], (first * LANES, (tall - first) * LANES - words))
    table = table.reshape(tall, LANES)
    tabs = spread(nx, table)
    flat = lambda a: a.reshape(-1, LANES)
    sums = local(nx, tuple(sections), row_counts, flat(date_key), flat(store_key), flat(product_key),
                 flat(revenue.astype(jnp.float32)), tabs)
    return join(nx, ny, sums)


def solution(mesh):
    rows = P(("gx", "gy"))
    return jax.shard_map(
        functools.partial(shards, mesh.shape["gx"], mesh.shape["gy"]),
        mesh=mesh,
        in_specs=(rows,) * 5 + (P("gx"),) * 5,
        out_specs=P(),
        check_vma=False,
    )
```

```python
import functools

import jax
import jax.numpy as jnp
from jax import lax
from jax.experimental import pallas as pl
from jax.experimental.pallas import tpu as pltpu
from jax.sharding import PartitionSpec as P

BRANDS = 1024
YEARS = 16
LANES = 128
CHAINS = 2
MESH = pl.DeviceIdType.MESH
VMEM = pl.BlockSpec(memory_space=pltpu.VMEM)
SMEM = pl.BlockSpec(memory_space=pltpu.SMEM)


def up(count, unit):
    return (count + unit - 1) // unit * unit


def flip(me, mask):
    out, bit = me, 1
    while bit <= mask:
        if mask & bit:
            out = out + bit * (1 - 2 * ((me // bit) % 2))
        bit *= 2
    return out


def spread_kernel(n, x_ref, o_ref, own_sem, send_sem, recv_sem):
    me = lax.axis_index("gx")
    half = x_ref.shape[0] // 2
    bits = n.bit_length() - 1
    rising = [1 << b for b in range(1, bits)]
    orders = (rising + [1], rising[::-1] + [1])
    barrier = pltpu.get_barrier_semaphore()
    for b in range(bits):
        pl.semaphore_signal(barrier, inc=1, device_id={"gx": flip(me, 1 << b)}, device_id_type=MESH)
    own = pltpu.make_async_copy(x_ref, o_ref.at[me], own_sem)
    own.start()
    pl.semaphore_wait(barrier, bits)

    def copy(h, mask, step):
        rows = pl.ds(h * half, half)
        slot = flip(me, mask)
        src = x_ref.at[rows] if mask == 0 else o_ref.at[slot, rows]
        return pltpu.make_async_remote_copy(
            src_ref=src,
            dst_ref=o_ref.at[slot, rows],
            send_sem=send_sem.at[h, mask + step],
            recv_sem=recv_sem.at[h, mask + step],
            device_id={"gx": flip(me, step)},
            device_id_type=MESH,
        )

    sent = []
    for h in range(2):
        for step in orders[h]:
            c = copy(h, 0, step)
            c.start()
            sent.append(c)
    arrivals = []
    for h in range(2):
        have = [0]
        listed = []
        for step in orders[h]:
            fresh = [m + step for m in have]
            listed += [(m, step) for m in fresh]
            have += fresh
        arrivals.append(listed)
    for pair in zip(*arrivals):
        for h, (mask, last) in enumerate(pair):
            copy(h, mask - last, last).wait_recv()
            for step in orders[h][orders[h].index(last) + 1:]:
                c = copy(h, mask, step)
                c.start()
                sent.append(c)
    for c in sent:
        c.wait_send()
    own.wait()


def spread(n, table):
    return pl.pallas_call(
        functools.partial(spread_kernel, n),
        out_shape=jax.ShapeDtypeStruct((n,) + table.shape, jnp.int32),
        in_specs=[VMEM],
        out_specs=VMEM,
        scratch_shapes=[
            pltpu.SemaphoreType.DMA,
            pltpu.SemaphoreType.DMA((2, n)),
            pltpu.SemaphoreType.DMA((2, n)),
        ],
        compiler_params=pltpu.CompilerParams(collective_id=0, has_side_effects=True),
    )(table)


DIMS = lax.GatherDimensionNumbers(
    offset_dims=(), collapsed_slice_dims=(1,), start_index_map=(1,),
    operand_batching_dims=(0,), start_indices_batching_dims=(0,),
)


def along_lanes(words, lane):
    return lax.gather(words, lane[..., None], DIMS, (1, 1), mode=lax.GatherScatterMode.PROMISE_IN_BOUNDS)


def pick(tab_ref, owner, base, rows, high, lane):
    lots = min(CHAINS, rows)
    parts = [jnp.zeros((8, LANES), jnp.int32) for _ in range(lots)]
    mine = high - owner * rows
    for r in range(rows):
        words = jnp.broadcast_to(tab_ref[owner, pl.ds(base + r, 1), :], (8, LANES))
        parts[r % lots] = jnp.where(mine == r, along_lanes(words, lane), parts[r % lots])
    while len(parts) > 1:
        parts = [a | b for a, b in zip(parts[::2], parts[1::2])] + parts[len(parts) // 2 * 2:]
    return parts[0]


def local_kernel(n, places, count_ref, date_ref, store_ref, product_ref, money_ref, all_ref, o_ref,
                 word_buf, money_buf, tab_ref, sems):
    tall = date_ref.shape[0]
    tiles = tall // 8
    (year_base, year_rows, year_words), (dflag_base, dflag_rows, dflag_words) = places[:2]
    (store_base, store_rows, store_words), (prod_base, prod_rows, prod_words) = places[2:4]
    brand_base, brand_rows, _ = places[4]

    small = pl.ds(prod_base, all_ref.shape[1] - prod_base)
    large = pl.ds(0, prod_base)
    fetches = [
        pltpu.make_async_copy(all_ref.at[:, part], tab_ref.at[:, part], sems.at[k])
        for k, part in enumerate((small, large))
    ]
    for f in fetches:
        f.start()
    fetches[0].wait()

    def where_is(k, shift, words, rows):
        w = lax.shift_right_logical(k, shift)
        owner = lax.shift_right_logical(w, words.bit_length() - 1)
        inside = w & (words - 1)
        return owner * rows + lax.shift_right_logical(inside, 7), inside & (LANES - 1)

    def look(keys, shift, base, rows, words):
        high, lane = where_is(keys, shift, words, rows)
        if n * rows <= 512:
            out = jnp.zeros((8, LANES), jnp.int32)
            for owner in range(n):
                out = out | pick(tab_ref, owner, base, rows, high, lane)
            return out
        return lax.fori_loop(
            0, n, lambda o, acc: acc | pick(tab_ref, o, base, rows, high, lane), jnp.zeros((8, LANES), jnp.int32)
        )

    count = count_ref[0]
    spot = lax.broadcasted_iota(jnp.int32, (8, LANES), 0) * LANES + lax.broadcasted_iota(
        jnp.int32, (8, LANES), 1
    )

    def filter_one(v):
        at = pl.ds(pl.multiple_of(v * 8, 8), 8)
        date, store, product = date_ref[at, :], store_ref[at, :], product_ref[at, :]
        year = lax.shift_right_logical(look(date, 3, year_base, year_rows, year_words), (date & 7) * 4) & 15
        passed = lax.shift_right_logical(look(date, 5, dflag_base, dflag_rows, dflag_words), date & 31)
        passed &= lax.shift_right_logical(look(store, 5, store_base, store_rows, store_words), store & 31)
        passed &= lax.shift_right_logical(look(product, 5, prod_base, prod_rows, prod_words), product & 31)
        live = spot + v * (8 * LANES) < count
        word_buf[at, :] = jnp.where(live & ((passed & 1) == 1), product | (year << 20), -1)

    both = 2 if tiles % 2 == 0 else 1

    def filter_tiles(v, carry):
        for k in range(both):
            filter_one(v * both + k)
        return carry

    lax.fori_loop(0, tiles // both, filter_tiles, 0)
    packed = word_buf[pl.ds(0, tall), :]
    keep = (packed >= 0).astype(jnp.int32)
    row = lax.broadcasted_iota(jnp.int32, (tall, LANES), 0)

    upto = keep
    step = 1
    while step < tall:
        upto = upto + jnp.where(row >= step, pltpu.roll(upto, step, 0), 0)
        step *= 2
    last = upto[tall - 8:, :]
    most = jnp.max(last + pltpu.roll(last, LANES // 2, 1))
    turns = (most + 15) // 16
    word = jnp.where(keep == 1, packed | ((row - upto + 1) << 24), -1)
    money = jnp.where(keep == 1, money_ref[...], 0.0)
    step, bit = 1, 24
    while step < tall:
        far_word = pltpu.roll(word, tall - step, 0)
        far_money = pltpu.roll(money, tall - step, 0)
        comes = (far_word >= 0) & ((far_word & (1 << bit)) != 0)
        leaves = (word & (1 << bit)) != 0
        word = jnp.where(comes, far_word, jnp.where(leaves, -1, word))
        money = jnp.where(comes, far_money, jnp.where(leaves, 0.0, money))
        step *= 2
        bit += 1
    word_buf[pl.ds(0, tall), :] = word
    money_buf[pl.ds(0, tall), :] = money
    word_buf[pl.ds(tall, 8), :] = jnp.full((8, LANES), -1, jnp.int32)
    money_buf[pl.ds(tall, 8), :] = jnp.zeros((8, LANES), jnp.float32)
    o_ref[...] = jnp.zeros_like(o_ref)
    fetches[1].wait()

    shard_bits = (prod_words * 32).bit_length() - 1
    group_row = lax.broadcasted_iota(jnp.int32, (LANES, LANES), 0)

    few = min(4, n)
    sub = lax.broadcasted_iota(jnp.int32, (8, LANES), 0)

    def mirror(x):
        x = pltpu.roll(x, LANES // 2, 1)
        for step in (1, 2, 4):
            x = jnp.where((sub & step) == 0, pltpu.roll(x, 8 - step, 0), pltpu.roll(x, step, 0))
        return x

    def group(g, carry):
        at = pl.ds(pl.multiple_of(g * 8, 8), 8)
        over = pl.ds(pl.multiple_of(jnp.minimum(2 * turns - 1 - g, tiles) * 8, 8), 8)
        w, cash = word_buf[at, :], money_buf[at, :]
        spare = w < 0
        w = jnp.where(spare, mirror(word_buf[over, :]), w)
        cash = jnp.where(spare, mirror(money_buf[over, :]), cash)
        key = w & 0xFFFFF
        owner = lax.shift_right_logical(key, shard_bits)
        inside = key & ((1 << shard_bits) - 1)
        third = ((inside.astype(jnp.float32) + 0.5) * (1.0 / 3.0)).astype(jnp.int32)
        shift = (inside - third * 3) * 10
        high = owner * brand_rows + lax.shift_right_logical(third, 7)
        lane = third & (LANES - 1)

        def owners(t, acc):
            for k in range(few):
                acc = acc | pick(tab_ref, t * few + k, brand_base, brand_rows, high, lane)
            return acc

        words = lax.fori_loop(0, n // few, owners, jnp.zeros((8, LANES), jnp.int32))
        brand = lax.shift_right_logical(words, shift) & 1023
        row_code = lax.shift_right_logical(brand, 7) * YEARS + (lax.shift_right_logical(w, 20) & 15)
        low = brand & (LANES - 1)
        left, right = [], []
        for s in range(8):
            left.append(jnp.where(group_row == row_code[s:s + 1], cash[s:s + 1], 0.0).astype(jnp.bfloat16))
            right.append(jnp.where(group_row == low[s:s + 1], 1.0, 0.0).astype(jnp.bfloat16))
        o_ref[...] += lax.dot_general(
            jnp.concatenate(left, axis=1), jnp.concatenate(right, axis=1),
            (((1,), (1,)), ((), ())), preferred_element_type=jnp.float32,
        )
        return carry

    lax.fori_loop(0, turns, group, 0)


def local(n, places, count, date, store, product, money, tables):
    tall = date.shape[0]
    return pl.pallas_call(
        functools.partial(local_kernel, n, places),
        out_shape=jax.ShapeDtypeStruct((LANES, LANES), jnp.float32),
        in_specs=[SMEM] + [VMEM] * 4 + [pl.BlockSpec(memory_space=pl.ANY)],
        out_specs=VMEM,
        scratch_shapes=[pltpu.VMEM((tall + 8, LANES), jnp.int32), pltpu.VMEM((tall + 8, LANES), jnp.float32),
            pltpu.VMEM(tables.shape, jnp.int32), pltpu.SemaphoreType.DMA((2,))],
    )(count, date, store, product, money, tables)


def join_kernel(nx, ny, x_ref, o_ref, in_x, part, in_y, whole, sx, rx, sy, ry, sz, rz):
    mx, my = lax.axis_index("gx"), lax.axis_index("gy")
    rows = part.shape[0]
    barrier = pltpu.get_barrier_semaphore()
    for d in range(1, nx):
        pl.semaphore_signal(barrier, inc=1, device_id={"gx": (mx + d) % nx}, device_id_type=MESH)
    for d in range(1, ny):
        pl.semaphore_signal(barrier, inc=1, device_id={"gy": (my + d) % ny}, device_id_type=MESH)
    pl.semaphore_wait(barrier, nx + ny - 2)

    def push(src, dst, send, recv, where):
        c = pltpu.make_async_remote_copy(
            src_ref=src, dst_ref=dst, send_sem=send, recv_sem=recv, device_id=where, device_id_type=MESH
        )
        c.start()
        return c

    first = []
    for d in range(1, nx):
        to = (mx + d) % nx
        first.append(push(x_ref.at[to], in_x.at[d - 1], sx.at[d - 1], rx.at[d - 1], {"gx": to}))
    total = x_ref[mx]
    for d, c in enumerate(first):
        c.wait_recv()
        total = total + in_x[d]
    part[...] = total
    second = []
    for d in range(1, ny):
        second.append(push(part, in_y.at[(my)], sy.at[d - 1], ry.at[d - 1], {"gy": (my + d) % ny}))
    for c in second:
        c.wait_recv()
    in_y[my] = total
    total = in_y[0]
    for d in range(1, ny):
        total = total + in_y[d]
    whole[mx] = total
    third = []
    for d in range(1, nx):
        third.append(push(whole.at[mx], whole.at[mx], sz.at[d - 1], rz.at[d - 1], {"gx": (mx + d) % nx}))
    for c in third:
        c.wait_recv()
    flat = whole[...].reshape(nx * rows, LANES)
    for j in range(BRANDS // LANES):
        o_ref[:, j * LANES:(j + 1) * LANES] = flat[j * YEARS:(j + 1) * YEARS]
    for c in first + second + third:
        c.wait_send()


def join(nx, ny, sums):
    rows = LANES // nx
    dma = pltpu.SemaphoreType.DMA
    return pl.pallas_call(
        functools.partial(join_kernel, nx, ny),
        out_shape=jax.ShapeDtypeStruct((YEARS, BRANDS), jnp.float32),
        in_specs=[VMEM],
        out_specs=VMEM,
        scratch_shapes=[
            pltpu.VMEM((nx - 1, rows, LANES), jnp.float32),
            pltpu.VMEM((rows, LANES), jnp.float32),
            pltpu.VMEM((ny, rows, LANES), jnp.float32),
            pltpu.VMEM((nx, rows, LANES), jnp.float32),
            dma((nx,)), dma((nx,)), dma((ny,)), dma((ny,)), dma((nx,)), dma((nx,)),
        ],
        compiler_params=pltpu.CompilerParams(collective_id=1, has_side_effects=True),
    )(sums.reshape(nx, rows, LANES))


def shards(nx, ny, date_key, store_key, product_key, revenue, row_counts,
           date_years, date_flags, store_flags, product_flags, brand_words):
    sections = [None] * 5
    base = 0
    tables = (date_years, date_flags, store_flags, product_flags, brand_words)
    for at in (4, 3, 2, 1, 0):
        words = tables[at].shape[0]
        rows = up(words, LANES) // LANES
        rows = up(rows, 8) if rows > 8 else rows
        sections[at] = (base, rows, words)
        base += rows
    tall = up(base, 16)
    table = jnp.zeros((tall * LANES,), jnp.int32)
    for at in range(5):
        first, _, words = sections[at]
        table = table | jnp.pad(tables[at], (first * LANES, (tall - first) * LANES - words))
    table = table.reshape(tall, LANES)
    tabs = spread(nx, table)
    flat = lambda a: a.reshape(-1, LANES)
    sums = local(nx, tuple(sections), row_counts, flat(date_key), flat(store_key), flat(product_key),
                 flat(revenue.astype(jnp.float32)), tabs)
    return join(nx, ny, sums)


def solution(mesh):
    rows = P(("gx", "gy"))
    return jax.shard_map(
        functools.partial(shards, mesh.shape["gx"], mesh.shape["gy"]),
        mesh=mesh,
        in_specs=(rows,) * 5 + (P("gx"),) * 5,
        out_specs=P(),
        check_vma=False,
    )
```

```python
import functools

import jax
import jax.numpy as jnp
from jax import lax
from jax.experimental import pallas as pl
from jax.experimental.pallas import tpu as pltpu
from jax.sharding import PartitionSpec as P

BRANDS = 1024
YEARS = 16
LANES = 128
CHAINS = 2
MESH = pl.DeviceIdType.MESH
VMEM = pl.BlockSpec(memory_space=pltpu.VMEM)
SMEM = pl.BlockSpec(memory_space=pltpu.SMEM)


def up(count, unit):
    return (count + unit - 1) // unit * unit


def flip(me, mask):
    out, bit = me, 1
    while bit <= mask:
        if mask & bit:
            out = out + bit * (1 - 2 * ((me // bit) % 2))
        bit *= 2
    return out


DIMS = lax.GatherDimensionNumbers(
    offset_dims=(), collapsed_slice_dims=(1,), start_index_map=(1,),
    operand_batching_dims=(0,), start_indices_batching_dims=(0,),
)


def along_lanes(words, lane):
    return lax.gather(words, lane[..., None], DIMS, (1, 1), mode=lax.GatherScatterMode.PROMISE_IN_BOUNDS)


def pick(tab_ref, owner, base, rows, high, lane):
    lots = min(CHAINS, rows)
    parts = [jnp.zeros((8, LANES), jnp.int32) for _ in range(lots)]
    mine = high - owner * rows
    for r in range(rows):
        words = jnp.broadcast_to(tab_ref[owner, pl.ds(base + r, 1), :], (8, LANES))
        parts[r % lots] = jnp.where(mine == r, along_lanes(words, lane), parts[r % lots])
    while len(parts) > 1:
        parts = [a | b for a, b in zip(parts[::2], parts[1::2])] + parts[len(parts) // 2 * 2:]
    return parts[0]


def filter_rows(n, places, count_ref, date_ref, store_ref, product_ref, near, word_ref):
    top = places[3][0]
    tiles = date_ref.shape[0] // 8
    (year_base, year_rows, year_words), (dflag_base, dflag_rows, dflag_words) = places[:2]
    (store_base, store_rows, store_words), (prod_base, prod_rows, prod_words) = places[2:4]

    def where_is(k, shift, words, rows):
        w = lax.shift_right_logical(k, shift)
        owner = lax.shift_right_logical(w, words.bit_length() - 1)
        inside = w & (words - 1)
        return owner * rows + lax.shift_right_logical(inside, 7), inside & (LANES - 1)

    def look(keys, shift, base, rows, words):
        high, lane = where_is(keys, shift, words, rows)
        if n * rows <= 512:
            out = jnp.zeros((8, LANES), jnp.int32)
            for owner in range(n):
                out = out | pick(near, owner, base - top, rows, high, lane)
            return out
        return lax.fori_loop(
            0, n, lambda o, acc: acc | pick(near, o, base - top, rows, high, lane), jnp.zeros((8, LANES), jnp.int32)
        )

    count = count_ref[0]
    spot = lax.broadcasted_iota(jnp.int32, (8, LANES), 0) * LANES + lax.broadcasted_iota(
        jnp.int32, (8, LANES), 1
    )

    def filter_one(v):
        at = pl.ds(pl.multiple_of(v * 8, 8), 8)
        date, store, product = date_ref[at, :], store_ref[at, :], product_ref[at, :]
        year = lax.shift_right_logical(look(date, 3, year_base, year_rows, year_words), (date & 7) * 4) & 15
        passed = lax.shift_right_logical(look(date, 5, dflag_base, dflag_rows, dflag_words), date & 31)
        passed &= lax.shift_right_logical(look(store, 5, store_base, store_rows, store_words), store & 31)
        passed &= lax.shift_right_logical(look(product, 5, prod_base, prod_rows, prod_words), product & 31)
        live = spot + v * (8 * LANES) < count
        word_ref[at, :] = jnp.where(live & ((passed & 1) == 1), product | (year << 20), -1)

    both = 2 if tiles % 2 == 0 else 1

    def filter_tiles(v, carry):
        for k in range(both):
            filter_one(v * both + k)
        return carry

    lax.fori_loop(0, tiles // both, filter_tiles, 0)


def spread_kernel(n, places, count_ref, date_ref, store_ref, product_ref, x_ref, o_ref, word_ref,
                  near, own_sem, send_sem, recv_sem):
    me = lax.axis_index("gx")
    top = o_ref.shape[1]
    cut = top // 16 * 8
    spans = ((top, near.shape[1], near), (0, cut, o_ref), (cut, top - cut, o_ref))
    bits = n.bit_length() - 1
    rising = [1 << b for b in range(1, bits)]
    orders = (rising + [1], rising + [1], rising[::-1] + [1])
    barrier = pltpu.get_barrier_semaphore()
    for b in range(bits):
        pl.semaphore_signal(barrier, inc=1, device_id={"gx": flip(me, 1 << b)}, device_id_type=MESH)
    owns = []
    for k, (first, rows, ref) in enumerate(((top, near.shape[1], near), (0, top, o_ref))):
        own = pltpu.make_async_copy(x_ref.at[pl.ds(first, rows)], ref.at[me], own_sem.at[k])
        own.start()
        owns.append(own)
    pl.semaphore_wait(barrier, bits)

    def copy(h, mask, step):
        first, rows, ref = spans[h]
        slot = flip(me, mask)
        dst = ref.at[slot] if h == 0 else ref.at[slot, pl.ds(first, rows)]
        return pltpu.make_async_remote_copy(
            src_ref=x_ref.at[pl.ds(first, rows)] if mask == 0 else dst,
            dst_ref=dst,
            send_sem=send_sem.at[h, mask + step],
            recv_sem=recv_sem.at[h, mask + step],
            device_id={"gx": flip(me, step)},
            device_id_type=MESH,
        )

    sent = []
    for h in range(3):
        for step in orders[h]:
            c = copy(h, 0, step)
            c.start()
            sent.append(c)
    arrivals = []
    for h in range(3):
        have = [0]
        listed = []
        for step in orders[h]:
            fresh = [m + step for m in have]
            listed += [(m, step) for m in fresh]
            have += fresh
        arrivals.append(listed)

    def arrive(h, mask, last):
        copy(h, mask - last, last).wait_recv()
        for step in orders[h][orders[h].index(last) + 1:]:
            c = copy(h, mask, step)
            c.start()
            sent.append(c)

    for mask, last in arrivals[0][:n // 2 - 1]:
        arrive(0, mask, last)
    early = 1 if n > 2 else 0
    for k in range(early):
        for h in (1, 2):
            arrive(h, *arrivals[h][k])
    for mask, last in arrivals[0][n // 2 - 1:]:
        arrive(0, mask, last)
    owns[0].wait()
    filter_rows(n, places, count_ref, date_ref, store_ref, product_ref, near, word_ref)
    for k in range(early, n - 1):
        for h in (1, 2):
            arrive(h, *arrivals[h][k])
    for c in sent:
        c.wait_send()
    owns[1].wait()


def spread(n, places, count, date, store, product, table):
    top, low = places[3][0], table.shape[0] - places[3][0]
    return pl.pallas_call(
        functools.partial(spread_kernel, n, places),
        out_shape=(
            jax.ShapeDtypeStruct((n, top, LANES), jnp.int32),
            jax.ShapeDtypeStruct(date.shape, jnp.int32),
        ),
        in_specs=[SMEM] + [VMEM] * 4,
        out_specs=(VMEM, VMEM),
        scratch_shapes=[
            pltpu.VMEM((n, low, LANES), jnp.int32),
            pltpu.SemaphoreType.DMA((2,)),
            pltpu.SemaphoreType.DMA((3, n)),
            pltpu.SemaphoreType.DMA((3, n)),
        ],
        compiler_params=pltpu.CompilerParams(collective_id=0, has_side_effects=True),
    )(count, date, store, product, table)


def local_kernel(n, places, packed_ref, money_ref, all_ref, o_ref, word_buf, money_buf, tab_ref, sem):
    tall = packed_ref.shape[0]
    tiles = tall // 8
    prod_words = places[3][2]
    brand_base, brand_rows, _ = places[4]
    fetch = pltpu.make_async_copy(all_ref, tab_ref, sem)
    fetch.start()
    packed = packed_ref[...]
    keep = (packed >= 0).astype(jnp.int32)
    row = lax.broadcasted_iota(jnp.int32, (tall, LANES), 0)

    upto = keep
    step = 1
    while step < tall:
        upto = upto + jnp.where(row >= step, pltpu.roll(upto, step, 0), 0)
        step *= 2
    last = upto[tall - 8:, :]
    most = jnp.max(last + pltpu.roll(last, LANES // 2, 1))
    turns = (most + 15) // 16
    word = jnp.where(keep == 1, packed | ((row - upto + 1) << 24), -1)
    money = jnp.where(keep == 1, money_ref[...], 0.0)
    step, bit = 1, 24
    while step < tall:
        far_word = pltpu.roll(word, tall - step, 0)
        far_money = pltpu.roll(money, tall - step, 0)
        comes = (far_word >= 0) & ((far_word & (1 << bit)) != 0)
        leaves = (word & (1 << bit)) != 0
        word = jnp.where(comes, far_word, jnp.where(leaves, -1, word))
        money = jnp.where(comes, far_money, jnp.where(leaves, 0.0, money))
        step *= 2
        bit += 1
    word_buf[pl.ds(0, tall), :] = word
    money_buf[pl.ds(0, tall), :] = money
    word_buf[pl.ds(tall, 8), :] = jnp.full((8, LANES), -1, jnp.int32)
    money_buf[pl.ds(tall, 8), :] = jnp.zeros((8, LANES), jnp.float32)
    o_ref[...] = jnp.zeros_like(o_ref)
    fetch.wait()

    shard_bits = (prod_words * 32).bit_length() - 1
    group_row = lax.broadcasted_iota(jnp.int32, (LANES, LANES), 0)

    few = min(4, n)
    sub = lax.broadcasted_iota(jnp.int32, (8, LANES), 0)

    def mirror(x):
        x = pltpu.roll(x, LANES // 2, 1)
        for step in (1, 2, 4):
            x = jnp.where((sub & step) == 0, pltpu.roll(x, 8 - step, 0), pltpu.roll(x, step, 0))
        return x

    def group(g, carry):
        at = pl.ds(pl.multiple_of(g * 8, 8), 8)
        over = pl.ds(pl.multiple_of(jnp.minimum(2 * turns - 1 - g, tiles) * 8, 8), 8)
        w, cash = word_buf[at, :], money_buf[at, :]
        spare = w < 0
        w = jnp.where(spare, mirror(word_buf[over, :]), w)
        cash = jnp.where(spare, mirror(money_buf[over, :]), cash)
        key = w & 0xFFFFF
        owner = lax.shift_right_logical(key, shard_bits)
        inside = key & ((1 << shard_bits) - 1)
        third = ((inside.astype(jnp.float32) + 0.5) * (1.0 / 3.0)).astype(jnp.int32)
        shift = (inside - third * 3) * 10
        high = owner * brand_rows + lax.shift_right_logical(third, 7)
        lane = third & (LANES - 1)

        def owners(t, acc):
            for k in range(few):
                acc = acc | pick(tab_ref, t * few + k, brand_base, brand_rows, high, lane)
            return acc

        words = lax.fori_loop(0, n // few, owners, jnp.zeros((8, LANES), jnp.int32))
        brand = lax.shift_right_logical(words, shift) & 1023
        row_code = lax.shift_right_logical(brand, 7) * YEARS + (lax.shift_right_logical(w, 20) & 15)
        low = brand & (LANES - 1)
        left, right = [], []
        for s in range(8):
            left.append(jnp.where(group_row == row_code[s:s + 1], cash[s:s + 1], 0.0).astype(jnp.bfloat16))
            right.append(jnp.where(group_row == low[s:s + 1], 1.0, 0.0).astype(jnp.bfloat16))
        o_ref[...] += lax.dot_general(
            jnp.concatenate(left, axis=1), jnp.concatenate(right, axis=1),
            (((1,), (1,)), ((), ())), preferred_element_type=jnp.float32,
        )
        return carry

    lax.fori_loop(0, turns, group, 0)


def local(n, places, packed, money, tables):
    tall = packed.shape[0]
    return pl.pallas_call(
        functools.partial(local_kernel, n, places),
        out_shape=jax.ShapeDtypeStruct((LANES, LANES), jnp.float32),
        in_specs=[VMEM, VMEM, pl.BlockSpec(memory_space=pl.ANY)],
        out_specs=VMEM,
        scratch_shapes=[
            pltpu.VMEM((tall + 8, LANES), jnp.int32), pltpu.VMEM((tall + 8, LANES), jnp.float32),
            pltpu.VMEM(tables.shape, jnp.int32), pltpu.SemaphoreType.DMA,
        ],
    )(packed, money, tables)


def join_kernel(nx, ny, x_ref, o_ref, in_x, part, in_y, whole, sx, rx, sy, ry, sz, rz):
    mx, my = lax.axis_index("gx"), lax.axis_index("gy")
    rows = part.shape[0]
    barrier = pltpu.get_barrier_semaphore()
    for d in range(1, nx):
        pl.semaphore_signal(barrier, inc=1, device_id={"gx": (mx + d) % nx}, device_id_type=MESH)
    for d in range(1, ny):
        pl.semaphore_signal(barrier, inc=1, device_id={"gy": (my + d) % ny}, device_id_type=MESH)
    pl.semaphore_wait(barrier, nx + ny - 2)

    def push(src, dst, send, recv, where):
        c = pltpu.make_async_remote_copy(
            src_ref=src, dst_ref=dst, send_sem=send, recv_sem=recv, device_id=where, device_id_type=MESH
        )
        c.start()
        return c

    first = []
    for d in range(1, nx):
        to = (mx + d) % nx
        first.append(push(x_ref.at[to], in_x.at[d - 1], sx.at[d - 1], rx.at[d - 1], {"gx": to}))
    total = x_ref[mx]
    for d, c in enumerate(first):
        c.wait_recv()
        total = total + in_x[d]
    part[...] = total
    second = []
    for d in range(1, ny):
        second.append(push(part, in_y.at[(my)], sy.at[d - 1], ry.at[d - 1], {"gy": (my + d) % ny}))
    for c in second:
        c.wait_recv()
    in_y[my] = total
    total = in_y[0]
    for d in range(1, ny):
        total = total + in_y[d]
    whole[mx] = total
    third = []
    for d in range(1, nx):
        third.append(push(whole.at[mx], whole.at[mx], sz.at[d - 1], rz.at[d - 1], {"gx": (mx + d) % nx}))
    for c in third:
        c.wait_recv()
    flat = whole[...].reshape(nx * rows, LANES)
    for j in range(BRANDS // LANES):
        o_ref[:, j * LANES:(j + 1) * LANES] = flat[j * YEARS:(j + 1) * YEARS]
    for c in first + second + third:
        c.wait_send()


def join(nx, ny, sums):
    rows = LANES // nx
    dma = pltpu.SemaphoreType.DMA
    return pl.pallas_call(
        functools.partial(join_kernel, nx, ny),
        out_shape=jax.ShapeDtypeStruct((YEARS, BRANDS), jnp.float32),
        in_specs=[VMEM],
        out_specs=VMEM,
        scratch_shapes=[
            pltpu.VMEM((nx - 1, rows, LANES), jnp.float32),
            pltpu.VMEM((rows, LANES), jnp.float32),
            pltpu.VMEM((ny, rows, LANES), jnp.float32),
            pltpu.VMEM((nx, rows, LANES), jnp.float32),
            dma((nx,)), dma((nx,)), dma((ny,)), dma((ny,)), dma((nx,)), dma((nx,)),
        ],
        compiler_params=pltpu.CompilerParams(collective_id=1, has_side_effects=True),
    )(sums.reshape(nx, rows, LANES))


def shards(nx, ny, date_key, store_key, product_key, revenue, row_counts,
           date_years, date_flags, store_flags, product_flags, brand_words):
    sections = [None] * 5
    base = 0
    tables = (date_years, date_flags, store_flags, product_flags, brand_words)
    for at in (4, 3, 2, 1, 0):
        words = tables[at].shape[0]
        rows = up(words, LANES) // LANES
        rows = up(rows, 8) if rows > 8 else rows
        sections[at] = (base, rows, words)
        base += rows
    tall = up(base, 16)
    table = jnp.zeros((tall * LANES,), jnp.int32)
    for at in range(5):
        first, _, words = sections[at]
        table = table | jnp.pad(tables[at], (first * LANES, (tall - first) * LANES - words))
    table = table.reshape(tall, LANES)
    places = tuple(sections)
    flat = lambda a: a.reshape(-1, LANES)
    tabs, packed = spread(nx, places, row_counts, flat(date_key), flat(store_key), flat(product_key), table)
    sums = local(nx, places, packed, flat(revenue.astype(jnp.float32)), tabs)
    return join(nx, ny, sums)


def solution(mesh):
    rows = P(("gx", "gy"))
    return jax.shard_map(
        functools.partial(shards, mesh.shape["gx"], mesh.shape["gy"]),
        mesh=mesh,
        in_specs=(rows,) * 5 + (P("gx"),) * 5,
        out_specs=P(),
        check_vma=False,
    )
```
